32 devices in a mesh: ctx: 8 (over z, x), heads: 4 (over y, core).
Axes of the slice: x: 2, y: 2, z: 4, core: 2. Of those that a mesh axis runs over, the one named last changes fastest.
Arguments:
- query_rows: bfloat16 [8, 16, 2, 128], P('ctx', 'heads'), may hold values from -6 to 6
- past_keys: bfloat16 [8, 16, 512, 128], P(None, 'heads', 'ctx'), may hold values from -6 to 6
- past_values: bfloat16 [8, 16, 512, 128], P(None, 'heads', 'ctx'), may hold values from -6 to 6
- used_length: int32 [8], replicated, may hold values from 256 to 512
Outputs:
- read: bfloat16 [8, 16, 2, 128], P('ctx', 'heads')
The draws below stay inside these ranges and needn't reach their ends.
All inputs are finite; a program needn't handle non-finite values.
Results may differ from the reference program's by a relative error of at most 0.0015.
Values may be sent and summed in bfloat16 or wider, within the bound.
A program may use at most 64 MiB of HBM per device.

```python
import jax
import jax.numpy as jnp
from jax import lax

BATCH = 8
LENGTH = 512
KV_HEADS = 16
GROUP = 2
HEAD_SIZE = 128


def set_ends(result, key, least, largest):
    place = [jax.random.randint(jax.random.fold_in(key, axis), (), 0, length) for axis, length in enumerate(result.shape)]
    main_axis = result.shape.index(max(result.shape))
    beside = place[:main_axis] + [(place[main_axis] + 1) % result.shape[main_axis]] + place[main_axis + 1:]
    return result.at[tuple(place)].set(least).at[tuple(beside)].set(largest)


def shard_levels(stream_key, extent, pieces, least, largest):
    def one(position, shards_of):
        draws = jax.random.uniform(jax.random.fold_in(jax.random.fold_in(stream_key, 6), position), (shards_of,), jnp.float32, least / len(pieces), largest / len(pieces))
        return jnp.repeat(jnp.exp(draws), extent[position] // shards_of).reshape((-1,) + (1,) * (len(extent) - position - 1))

    factor_of = one(*pieces[0])
    for cut in pieces[1:]:
        factor_of = factor_of * one(*cut)
    return factor_of


def gaussian(rng, shape, width, most, cuts=(), kind=jnp.bfloat16):
    drawn = width * jax.random.normal(rng, shape, jnp.float32)
    if cuts:
        drawn = drawn * shard_levels(rng, shape, cuts, -0.22, 0.18)
    return jnp.clip(drawn, -most, most).astype(kind)


def setup_inputs(seed: int = 0) -> dict:
    key_of = jax.random.split(jax.random.key(seed), 5)
    query_rows = gaussian(key_of[0], (BATCH, KV_HEADS, GROUP, HEAD_SIZE), 1.0, 6.0, ((0, 8), (1, 4)))
    past_keys = gaussian(key_of[1], (BATCH, KV_HEADS, LENGTH, HEAD_SIZE), 1.0, 6.0, ((1, 4), (2, 8)))
    past_values = gaussian(key_of[2], (BATCH, KV_HEADS, LENGTH, HEAD_SIZE), 1.0, 6.0, ((1, 4), (2, 8)))
    used_length = set_ends(jax.random.randint(key_of[3], (BATCH,), LENGTH // 2, LENGTH + 1), jax.random.fold_in(key_of[3], 1), LENGTH // 2, LENGTH).astype(jnp.int32)
    return dict(query_rows=query_rows, past_keys=past_keys, past_values=past_values, used_length=used_length)


def reference(query_rows, past_keys, past_values, used_length):
    def one_sequence(item):
        query_one, keys_one, values_one, length_one = item
        logit = jnp.einsum("kgd,ktd->kgt", query_one.astype(jnp.float32), keys_one.astype(jnp.float32)) * HEAD_SIZE ** -0.5
        logit = jnp.where(jnp.arange(LENGTH) < length_one, logit, -1e30)
        share = jax.nn.softmax(logit, axis=-1)
        return jnp.einsum("kgt,ktd->kgd", share, values_one.astype(jnp.float32), precision=lax.Precision.HIGHEST)
    read = lax.map(one_sequence, (query_rows, past_keys, past_values, used_length)).astype(jnp.bfloat16)
    return read
```

```python
import functools

import jax
import jax.numpy as jnp
from jax import lax
from jax.experimental import pallas as pl
from jax.experimental.pallas import tpu as pltpu
from jax.sharding import PartitionSpec as P

MESH = pl.DeviceIdType.MESH


def partner(me, step, n):
    if n & (n - 1):
        return lax.rem(me + step, n), lax.rem(me + n - step, n)
    peer, bit = 0, 1
    while bit < n:
        own = lax.rem(me // bit, 2)
        peer = peer + bit * (1 - own if step & bit else own)
        bit *= 2
    return peer, peer


def groups_of(n):
    groups, start = [[0]], 1
    while start < n:
        groups.append(list(range(start, min(2 * start + 2, n))))
        start = groups[-1][-1] + 1
    return groups


def kernel(
    n, per, heads, group, scale,
    q_hbm, k_hbm, v_hbm, length_hbm, out_ref,
    queries, keys, values, length, sent, landed,
    local_sem, q_send, q_recv, part_send, part_recv,
):
    me = lax.axis_index("ctx")
    rows = heads * group
    width = keys.shape[1]
    stretch = width // heads
    to = [partner(me, s, n)[0] for s in range(n)]
    source = [partner(me, s, n)[1] for s in range(n)]

    local = [
        pltpu.make_async_copy(q_hbm, queries.at[0], local_sem.at[0]),
        pltpu.make_async_copy(length_hbm, length, local_sem.at[1]),
        pltpu.make_async_copy(k_hbm, keys, local_sem.at[2]),
        pltpu.make_async_copy(v_hbm, values, local_sem.at[3]),
    ]
    barrier = pltpu.get_barrier_semaphore()
    for s in range(n - 1, 0, -1):
        pl.semaphore_signal(barrier, inc=1, device_id={"ctx": to[s]}, device_id_type=MESH)
    for copy in local:
        copy.start()
    local[0].wait()
    pl.semaphore_wait(barrier, n - 1)

    asked = {}
    for s in range(n - 1, 0, -1):
        asked[s] = pltpu.make_async_remote_copy(
            src_ref=queries.at[0], dst_ref=queries.at[s],
            send_sem=q_send.at[s], recv_sem=q_recv.at[s],
            device_id={"ctx": to[s]}, device_id_type=MESH,
        )
        asked[s].start()
    for copy in local[1:]:
        copy.wait()

    row = lax.broadcasted_iota(jnp.int32, (rows, width), 0)
    column = lax.broadcasted_iota(jnp.int32, (rows, width), 1)
    same_head = (row // group) == (column // stretch)
    position = me * stretch + lax.rem(column, stretch)
    left = lax.broadcasted_iota(jnp.int32, (rows, 128), 1) < 64
    answers = {}
    for steps in groups_of(n):
        for s in steps:
            if s:
                asked[s].wait_recv()
        for s in steps:
            for j in range(per):
                b = source[s] * per + j
                logit = lax.dot_general(
                    queries[s, j], keys[b], (((1,), (1,)), ((), ())),
                    preferred_element_type=jnp.float32,
                ) * scale
                filled = same_head & (position < length[b])
                logit = jnp.where(filled, logit, -1e30)
                top = jnp.max(logit, axis=-1, keepdims=True)
                part = jnp.where(filled, jnp.exp(logit - top), 0.0)
                weight = jnp.sum(part, axis=-1, keepdims=True)
                high = part.astype(jnp.bfloat16)
                low = (part - high.astype(jnp.float32)).astype(jnp.bfloat16)
                both = jnp.dot(
                    jnp.concatenate([high, low], axis=0), values[b],
                    preferred_element_type=jnp.float32,
                )
                slot = sent if s else landed
                slot[s, j, :rows] = both[:rows] + both[rows:]
                slot[s, j, rows:] = jnp.where(left, top, weight)
        for s in steps:
            if s:
                answers[s] = pltpu.make_async_remote_copy(
                    src_ref=sent.at[s], dst_ref=landed.at[s],
                    send_sem=part_send.at[s], recv_sem=part_recv.at[s],
                    device_id={"ctx": source[s]}, device_id_type=MESH,
                )
                answers[s].start()
    for s in range(1, n):
        answers[s].wait_recv()
    for j in range(per):
        tops = [landed[s, j, rows:, 0:1] for s in range(n)]
        weights = [landed[s, j, rows:, 64:65] for s in range(n)]
        best = functools.reduce(jnp.maximum, tops)
        scales = [jnp.exp(top - best) for top in tops]
        total = sum(weight * by for weight, by in zip(weights, scales))
        read = sum(landed[s, j, :rows] * scales[s] for s in range(n))
        out_ref[j * rows:(j + 1) * rows] = (read / total).astype(out_ref.dtype)
    for s in range(1, n):
        asked[s].wait_send()
        answers[s].wait_send()


def solution(mesh):
    n = mesh.shape["ctx"]

    def local(query_rows, past_keys, past_values, used_length):
        per, heads, group, size = query_rows.shape
        batch, _, stretch, _ = past_keys.shape
        rows, width = heads * group, heads * stretch
        any_space = pl.BlockSpec(memory_space=pl.ANY)
        out = pl.pallas_call(
            functools.partial(kernel, n, per, heads, group, size ** -0.5),
            out_shape=jax.ShapeDtypeStruct((per * rows, size), query_rows.dtype),
            in_specs=[any_space] * 4,
            out_specs=pl.BlockSpec(memory_space=pltpu.VMEM),
            scratch_shapes=[
                pltpu.VMEM((n, per, rows, size), query_rows.dtype),
                pltpu.VMEM((batch, width, size), past_keys.dtype),
                pltpu.VMEM((batch, width, size), past_values.dtype),
                pltpu.SMEM((batch,), jnp.int32),
                pltpu.VMEM((n, per, 2 * rows, size), jnp.float32),
                pltpu.VMEM((n, per, 2 * rows, size), jnp.float32),
                pltpu.SemaphoreType.DMA((4,)),
                pltpu.SemaphoreType.DMA((n,)),
                pltpu.SemaphoreType.DMA((n,)),
                pltpu.SemaphoreType.DMA((n,)),
                pltpu.SemaphoreType.DMA((n,)),
            ],
            compiler_params=pltpu.CompilerParams(collective_id=0, has_side_effects=True),
        )(
            query_rows.reshape(per, rows, size),
            past_keys.reshape(batch, width, size),
            past_values.reshape(batch, width, size),
            used_length,
        )
        return out.reshape(query_rows.shape)

    return jax.shard_map(
        local,
        mesh=mesh,
        in_specs=(
            P("ctx", "heads", None, None),
            P(None, "heads", "ctx", None),
            P(None, "heads", "ctx", None),
            P(),
        ),
        out_specs=P("ctx", "heads", None, None),
        check_vma=False,
    )
```

```python
import functools

import jax
import jax.numpy as jnp
from jax import lax
from jax.experimental import pallas as pl
from jax.experimental.pallas import tpu as pltpu
from jax.sharding import PartitionSpec as P

MESH = pl.DeviceIdType.MESH


def partner(me, step, n):
    if n & (n - 1):
        return lax.rem(me + step, n), lax.rem(me + n - step, n)
    peer, bit = 0, 1
    while bit < n:
        own = lax.rem(me // bit, 2)
        peer = peer + bit * (1 - own if step & bit else own)
        bit *= 2
    return peer, peer


def groups_of(n):
    return [[s] for s in range(n)]


def kernel(
    n, per, heads, group, scale,
    q_hbm, k_hbm, v_hbm, length_hbm, out_ref,
    queries, keys, values, length, sent, landed,
    local_sem, q_send, q_recv, part_send, part_recv,
):
    me = lax.axis_index("ctx")
    rows = heads * group
    width = keys.shape[1]
    stretch = width // heads
    to = [partner(me, s, n)[0] for s in range(n)]
    source = [partner(me, s, n)[1] for s in range(n)]

    local = [
        pltpu.make_async_copy(q_hbm, queries.at[0], local_sem.at[0]),
        pltpu.make_async_copy(length_hbm, length, local_sem.at[1]),
        pltpu.make_async_copy(k_hbm, keys, local_sem.at[2]),
        pltpu.make_async_copy(v_hbm, values, local_sem.at[3]),
    ]
    barrier = pltpu.get_barrier_semaphore()
    for s in range(n - 1, 0, -1):
        pl.semaphore_signal(barrier, inc=1, device_id={"ctx": to[s]}, device_id_type=MESH)
    for copy in local:
        copy.start()
    local[0].wait()
    pl.semaphore_wait(barrier, n - 1)

    asked = {}
    for s in range(n - 1, 0, -1):
        asked[s] = pltpu.make_async_remote_copy(
            src_ref=queries.at[0], dst_ref=queries.at[s],
            send_sem=q_send.at[s], recv_sem=q_recv.at[s],
            device_id={"ctx": to[s]}, device_id_type=MESH,
        )
        asked[s].start()
    for copy in local[1:]:
        copy.wait()

    row = lax.broadcasted_iota(jnp.int32, (rows, width), 0)
    column = lax.broadcasted_iota(jnp.int32, (rows, width), 1)
    same_head = (row // group) == (column // stretch)
    position = me * stretch + lax.rem(column, stretch)
    left = lax.broadcasted_iota(jnp.int32, (rows, 128), 1) < 64
    answers = {}
    for steps in groups_of(n):
        for s in steps:
            if s:
                asked[s].wait_recv()
        for s in steps:
            for j in range(per):
                b = source[s] * per + j
                logit = lax.dot_general(
                    queries[s, j], keys[b], (((1,), (1,)), ((), ())),
                    preferred_element_type=jnp.float32,
                ) * scale
                filled = same_head & (position < length[b])
                logit = jnp.where(filled, logit, -1e30)
                top = jnp.max(logit, axis=-1, keepdims=True)
                part = jnp.where(filled, jnp.exp(logit - top), 0.0)
                weight = jnp.sum(part, axis=-1, keepdims=True)
                high = part.astype(jnp.bfloat16)
                low = (part - high.astype(jnp.float32)).astype(jnp.bfloat16)
                both = jnp.dot(
                    jnp.concatenate([high, low], axis=0), values[b],
                    preferred_element_type=jnp.float32,
                )
                slot = sent if s else landed
                slot[s, j, :rows] = both[:rows] + both[rows:]
                slot[s, j, rows:] = jnp.where(left, top, weight)
        for s in steps:
            if s:
                answers[s] = pltpu.make_async_remote_copy(
                    src_ref=sent.at[s], dst_ref=landed.at[s],
                    send_sem=part_send.at[s], recv_sem=part_recv.at[s],
                    device_id={"ctx": source[s]}, device_id_type=MESH,
                )
                answers[s].start()
    for s in range(1, n):
        answers[s].wait_recv()
    for j in range(per):
        tops = [landed[s, j, rows:, 0:1] for s in range(n)]
        weights = [landed[s, j, rows:, 64:65] for s in range(n)]
        best = functools.reduce(jnp.maximum, tops)
        scales = [jnp.exp(top - best) for top in tops]
        total = sum(weight * by for weight, by in zip(weights, scales))
        read = sum(landed[s, j, :rows] * scales[s] for s in range(n))
        out_ref[j * rows:(j + 1) * rows] = (read / total).astype(out_ref.dtype)
    for s in range(1, n):
        asked[s].wait_send()
        answers[s].wait_send()


def solution(mesh):
    n = mesh.shape["ctx"]

    def local(query_rows, past_keys, past_values, used_length):
        per, heads, group, size = query_rows.shape
        batch, _, stretch, _ = past_keys.shape
        rows, width = heads * group, heads * stretch
        any_space = pl.BlockSpec(memory_space=pl.ANY)
        out = pl.pallas_call(
            functools.partial(kernel, n, per, heads, group, size ** -0.5),
            out_shape=pltpu.VMEM((per * rows, size), query_rows.dtype),
            in_specs=[any_space] * 4,
            out_specs=pl.BlockSpec(memory_space=pltpu.VMEM),
            scratch_shapes=[
                pltpu.VMEM((n, per, rows, size), query_rows.dtype),
                pltpu.VMEM((batch, width, size), past_keys.dtype),
                pltpu.VMEM((batch, width, size), past_values.dtype),
                pltpu.SMEM((batch,), jnp.int32),
                pltpu.VMEM((n, per, 2 * rows, size), jnp.float32),
                pltpu.VMEM((n, per, 2 * rows, size), jnp.float32),
                pltpu.SemaphoreType.DMA((4,)),
                pltpu.SemaphoreType.DMA((n,)),
                pltpu.SemaphoreType.DMA((n,)),
                pltpu.SemaphoreType.DMA((n,)),
                pltpu.SemaphoreType.DMA((n,)),
            ],
            compiler_params=pltpu.CompilerParams(collective_id=0, has_side_effects=True),
        )(
            query_rows.reshape(per, rows, size),
            past_keys.reshape(batch, width, size),
            past_values.reshape(batch, width, size),
            used_length,
        )
        return out.reshape(query_rows.shape)

    return jax.shard_map(
        local,
        mesh=mesh,
        in_specs=(
            P("ctx", "heads", None, None),
            P(None, "heads", "ctx", None),
            P(None, "heads", "ctx", None),
            P(),
        ),
        out_specs=P("ctx", "heads", None, None),
        check_vma=False,
    )
```

```python
import functools

import jax
import jax.numpy as jnp
from jax import lax
from jax.experimental import pallas as pl
from jax.experimental.pallas import tpu as pltpu
from jax.sharding import PartitionSpec as P

MESH = pl.DeviceIdType.MESH


def partner(me, step, n):
    if n & (n - 1):
        return lax.rem(me + step, n), lax.rem(me + n - step, n)
    peer, bit = 0, 1
    while bit < n:
        own = lax.rem(me // bit, 2)
        peer = peer + bit * (1 - own if step & bit else own)
        bit *= 2
    return peer, peer


def reach(n):
    if n & (n - 1):
        return n
    near = 1
    while near * near < n:
        near *= 2
    return near


def kernel(
    n, per, heads, group, scale,
    q_hbm, k_hbm, v_hbm, length_hbm, out_ref,
    queries, keys, values, length, sent, landed,
    local_sem, q_send, q_recv, part_send, part_recv,
):
    me = lax.axis_index("ctx")
    rows = heads * group
    width = keys.shape[1]
    stretch = width // heads
    to = [partner(me, s, n)[0] for s in range(n)]
    source = [partner(me, s, n)[1] for s in range(n)]

    local = [
        pltpu.make_async_copy(q_hbm, queries.at[0], local_sem.at[0]),
        pltpu.make_async_copy(length_hbm, length, local_sem.at[1]),
        pltpu.make_async_copy(k_hbm, keys, local_sem.at[2]),
        pltpu.make_async_copy(v_hbm, values, local_sem.at[3]),
    ]
    barrier = pltpu.get_barrier_semaphore()
    near = reach(n)
    far = list(range(near, n, near))
    direct = far + list(range(near - 1, 0, -1))
    for s in direct:
        pl.semaphore_signal(barrier, inc=1, device_id={"ctx": to[s]}, device_id_type=MESH)
    for copy in local:
        copy.start()
    local[0].wait()
    pl.semaphore_wait(barrier, len(direct))

    asked = {}

    def ask(slot, target, origin):
        asked[slot] = pltpu.make_async_remote_copy(
            src_ref=queries.at[origin], dst_ref=queries.at[slot],
            send_sem=q_send.at[slot], recv_sem=q_recv.at[slot],
            device_id={"ctx": to[target]}, device_id_type=MESH,
        )
        asked[slot].start()

    for s in direct:
        ask(s, s, 0)
    for copy in local[1:]:
        copy.wait()

    row = lax.broadcasted_iota(jnp.int32, (rows, width), 0)
    column = lax.broadcasted_iota(jnp.int32, (rows, width), 1)
    same_head = (row // group) == (column // stretch)
    position = me * stretch + lax.rem(column, stretch)
    left = lax.broadcasted_iota(jnp.int32, (rows, 128), 1) < 64
    answers = {}

    def answer(s):
        for j in range(per):
            b = source[s] * per + j
            logit = lax.dot_general(
                queries[s, j], keys[b], (((1,), (1,)), ((), ())),
                preferred_element_type=jnp.float32,
            ) * scale
            filled = same_head & (position < length[b])
            logit = jnp.where(filled, logit, -1e30)
            top = jnp.max(logit, axis=-1, keepdims=True)
            part = jnp.where(filled, jnp.exp(logit - top), 0.0)
            weight = jnp.sum(part, axis=-1, keepdims=True)
            high = part.astype(jnp.bfloat16)
            low = (part - high.astype(jnp.float32)).astype(jnp.bfloat16)
            both = jnp.dot(
                jnp.concatenate([high, low], axis=0), values[b],
                preferred_element_type=jnp.float32,
            )
            slot = sent if s else landed
            slot[s, j, :rows] = both[:rows] + both[rows:]
            slot[s, j, rows:] = jnp.where(left, top, weight)
        if s:
            answers[s] = pltpu.make_async_remote_copy(
                src_ref=sent.at[s], dst_ref=landed.at[s],
                send_sem=part_send.at[s], recv_sem=part_recv.at[s],
                device_id={"ctx": source[s]}, device_id_type=MESH,
            )
            answers[s].start()

    answer(0)
    for high in far:
        asked[high].wait_recv()
        for low in range(near - 1, 0, -1):
            ask(high + low, low, high)
    for s in range(1, near):
        asked[s].wait_recv()
        answer(s)
    for high in far:
        answer(high)
        for low in range(1, near):
            asked[high + low].wait_recv()
            answer(high + low)
    for s in range(1, n):
        answers[s].wait_recv()
    for j in range(per):
        tops = [landed[s, j, rows:, 0:1] for s in range(n)]
        weights = [landed[s, j, rows:, 64:65] for s in range(n)]
        best = functools.reduce(jnp.maximum, tops)
        scales = [jnp.exp(top - best) for top in tops]
        total = sum(weight * by for weight, by in zip(weights, scales))
        read = sum(landed[s, j, :rows] * scales[s] for s in range(n))
        out_ref[j * rows:(j + 1) * rows] = (read / total).astype(out_ref.dtype)
    for s in range(1, n):
        asked[s].wait_send()
        answers[s].wait_send()


def solution(mesh):
    n = mesh.shape["ctx"]

    def local(query_rows, past_keys, past_values, used_length):
        per, heads, group, size = query_rows.shape
        batch, _, stretch, _ = past_keys.shape
        rows, width = heads * group, heads * stretch
        any_space = pl.BlockSpec(memory_space=pl.ANY)
        out = pl.pallas_call(
            functools.partial(kernel, n, per, heads, group, size ** -0.5),
            out_shape=pltpu.VMEM((per * rows, size), query_rows.dtype),
            in_specs=[any_space] * 4,
            out_specs=pl.BlockSpec(memory_space=pltpu.VMEM),
            scratch_shapes=[
                pltpu.VMEM((n, per, rows, size), query_rows.dtype),
                pltpu.VMEM((batch, width, size), past_keys.dtype),
                pltpu.VMEM((batch, width, size), past_values.dtype),
                pltpu.SMEM((batch,), jnp.int32),
                pltpu.VMEM((n, per, 2 * rows, size), jnp.float32),
                pltpu.VMEM((n, per, 2 * rows, size), jnp.float32),
                pltpu.SemaphoreType.DMA((4,)),
                pltpu.SemaphoreType.DMA((n,)),
                pltpu.SemaphoreType.DMA((n,)),
                pltpu.SemaphoreType.DMA((n,)),
                pltpu.SemaphoreType.DMA((n,)),
            ],
            compiler_params=pltpu.CompilerParams(collective_id=0, has_side_effects=True),
        )(
            query_rows.reshape(per, rows, size),
            past_keys.reshape(batch, width, size),
            past_values.reshape(batch, width, size),
            used_length,
        )
        return out.reshape(query_rows.shape)

    return jax.shard_map(
        local,
        mesh=mesh,
        in_specs=(
            P("ctx", "heads", None, None),
            P(None, "heads", "ctx", None),
            P(None, "heads", "ctx", None),
            P(),
        ),
        out_specs=P("ctx", "heads", None, None),
        check_vma=False,
    )
```

```python
import functools

import jax
import jax.numpy as jnp
from jax import lax
from jax.experimental import pallas as pl
from jax.experimental.pallas import tpu as pltpu
from jax.sharding import PartitionSpec as P

MESH = pl.DeviceIdType.MESH


def partner(me, step, n):
    if n & (n - 1):
        return lax.rem(me + step, n), lax.rem(me + n - step, n)
    peer, bit = 0, 1
    while bit < n:
        own = lax.rem(me // bit, 2)
        peer = peer + bit * (1 - own if step & bit else own)
        bit *= 2
    return peer, peer


def groups_of(n):
    return [[s] for s in range(n)]


def kernel(
    n, per, heads, group, scale,
    q_hbm, k_hbm, v_hbm, length_hbm, out_ref,
    queries, keys, values, length, sent, landed,
    local_sem, q_send, q_recv, part_send, part_recv,
):
    me = lax.axis_index("ctx")
    rows = heads * group
    width = keys.shape[1]
    stretch = width // heads
    to = [partner(me, s, n)[0] for s in range(n)]
    source = [partner(me, s, n)[1] for s in range(n)]

    local = [
        pltpu.make_async_copy(q_hbm, queries.at[0], local_sem.at[0]),
        pltpu.make_async_copy(length_hbm, length, local_sem.at[1]),
        pltpu.make_async_copy(k_hbm, keys, local_sem.at[2]),
        pltpu.make_async_copy(v_hbm, values, local_sem.at[3]),
    ]
    barrier = pltpu.get_barrier_semaphore()
    for s in range(n - 1, 0, -1):
        pl.semaphore_signal(barrier, inc=1, device_id={"ctx": to[s]}, device_id_type=MESH)
    for copy in local:
        copy.start()
    local[0].wait()
    pl.semaphore_wait(barrier, n - 1)

    asked = {}
    for s in range(n - 1, 0, -1):
        asked[s] = pltpu.make_async_remote_copy(
            src_ref=queries.at[0], dst_ref=queries.at[s],
            send_sem=q_send.at[s], recv_sem=q_recv.at[s],
            device_id={"ctx": to[s]}, device_id_type=MESH,
        )
        asked[s].start()
    for copy in local[1:]:
        copy.wait()

    row = lax.broadcasted_iota(jnp.int32, (rows, width), 0)
    column = lax.broadcasted_iota(jnp.int32, (rows, width), 1)
    same_head = (row // group) == (column // stretch)
    position = me * stretch + lax.rem(column, stretch)
    filled = {
        (s, j): same_head & (position < length[source[s] * per + j])
        for s in range(n) for j in range(per)
    }
    answers = {}
    for steps in groups_of(n):
        for s in steps:
            if s:
                asked[s].wait_recv()
        for s in steps:
            for j in range(per):
                b = source[s] * per + j
                logit = lax.dot_general(
                    queries[s, j], keys[b], (((1,), (1,)), ((), ())),
                    preferred_element_type=jnp.float32,
                ) * scale
                logit = jnp.where(filled[s, j], logit, -1e30)
                top = jnp.max(logit, axis=-1, keepdims=True)
                part = jnp.where(filled[s, j], jnp.exp(logit - top), 0.0)
                weight = jnp.maximum(jnp.sum(part, axis=-1, keepdims=True), 1.0)
                inverse = 1.0 / weight
                level = top + jnp.log(weight)
                high = part.astype(jnp.bfloat16)
                low = (part - high.astype(jnp.float32)).astype(jnp.bfloat16)
                both = jnp.dot(
                    jnp.concatenate([high, low], axis=0), values[b],
                    preferred_element_type=jnp.float32,
                )
                slot = sent if s else landed
                slot[s, j, :rows] = (both[:rows] + both[rows:]) * inverse
                slot[s, j, rows:] = jnp.broadcast_to(level, (rows, both.shape[1]))
        for s in steps:
            if s:
                answers[s] = pltpu.make_async_remote_copy(
                    src_ref=sent.at[s], dst_ref=landed.at[s],
                    send_sem=part_send.at[s], recv_sem=part_recv.at[s],
                    device_id={"ctx": source[s]}, device_id_type=MESH,
                )
                answers[s].start()
    best = [landed[0, j, rows:] for j in range(per)]
    read = [landed[0, j, :rows] for j in range(per)]
    total = [jnp.ones_like(x) for x in best]
    for s in range(1, n):
        answers[s].wait_recv()
        for j in range(per):
            level = landed[s, j, rows:]
            higher = jnp.maximum(best[j], level)
            old, new = jnp.exp(best[j] - higher), jnp.exp(level - higher)
            read[j] = read[j] * old + landed[s, j, :rows] * new
            total[j] = total[j] * old + new
            best[j] = higher
    for j in range(per):
        out_ref[j * rows:(j + 1) * rows] = (read[j] / total[j]).astype(out_ref.dtype)
    for s in range(1, n):
        asked[s].wait_send()
        answers[s].wait_send()


def solution(mesh):
    n = mesh.shape["ctx"]

    def local(query_rows, past_keys, past_values, used_length):
        per, heads, group, size = query_rows.shape
        batch, _, stretch, _ = past_keys.shape
        rows, width = heads * group, heads * stretch
        any_space = pl.BlockSpec(memory_space=pl.ANY)
        out = pl.pallas_call(
            functools.partial(kernel, n, per, heads, group, size ** -0.5),
            out_shape=pltpu.VMEM((per * rows, size), query_rows.dtype),
            in_specs=[any_space] * 4,
            out_specs=pl.BlockSpec(memory_space=pltpu.VMEM),
            scratch_shapes=[
                pltpu.VMEM((n, per, rows, size), query_rows.dtype),
                pltpu.VMEM((batch, width, size), past_keys.dtype),
                pltpu.VMEM((batch, width, size), past_values.dtype),
                pltpu.SMEM((batch,), jnp.int32),
                pltpu.VMEM((n, per, 2 * rows, size), jnp.float32),
                pltpu.VMEM((n, per, 2 * rows, size), jnp.float32),
                pltpu.SemaphoreType.DMA((4,)),
                pltpu.SemaphoreType.DMA((n,)),
                pltpu.SemaphoreType.DMA((n,)),
                pltpu.SemaphoreType.DMA((n,)),
                pltpu.SemaphoreType.DMA((n,)),
            ],
            compiler_params=pltpu.CompilerParams(collective_id=0, has_side_effects=True),
        )(
            query_rows.reshape(per, rows, size),
            past_keys.reshape(batch, width, size),
            past_values.reshape(batch, width, size),
            used_length,
        )
        return out.reshape(query_rows.shape)

    return jax.shard_map(
        local,
        mesh=mesh,
        in_specs=(
            P("ctx", "heads", None, None),
            P(None, "heads", "ctx", None),
            P(None, "heads", "ctx", None),
            P(),
        ),
        out_specs=P("ctx", "heads", None, None),
        check_vma=False,
    )
```
